32 devices in a mesh: shot: 2 (over y), gx: 4 (over z), gy: 4 (over x, core).
Axes of the slice: x: 2, y: 2, z: 4, core: 2. Of those that a mesh axis runs over, the one named last changes fastest.
Arguments:
- wavefield: float32 [9, 64, 64, 128], P(None, ('shot', 'gx'), 'gy'), parts along dimension 1, may hold values from -10 to 10
- labels: int32 [32, 64, 128], P('gx', 'gy'), may hold values from 0 to 7
- lame_table: float32 [8], replicated, may hold values from 0.5 to 2
- shear_table: float32 [8], replicated, may hold values from 0.1 to 0.6
- density_table: float32 [8], replicated, may hold values from 0.8 to 2
- source_cells: int32 [128], P('shot'), parts along dimension 0, may hold values from 0 to 262143
- source_amps: float32 [5, 128], P(None, 'shot'), parts along dimension 1, may hold values from -6 to 6
- receiver_cells: int32 [256], replicated, may hold values from 0 to 262143
Outputs:
- final_fields: float32 [9, 64, 64, 128], P(None, ('shot', 'gx'), 'gy'), parts along dimension 1
- traces: float32 [5, 512], P(None, 'shot'), parts along dimension 1
The draws below stay inside these ranges and needn't reach their ends.
There are 2 independent parts, one for each index of `shot`. The reference program is written for one: setup_inputs(seed, part) draws one part's arguments, and reference() takes and returns one part's arrays. A program takes and returns all parts, laid end to end along the dimension named above; an argument that names none is the same for every part. Nothing has to cross between parts.
Inputs may be any that keep to these rules, and one draw needn't show every extreme that they name: `source_cells`: a flat cell index, x slowest, z fastest. `receiver_cells`: a flat cell index, x slowest, z fastest.
All inputs are finite; a program needn't handle non-finite values.
Results may differ from the reference program's by a relative error of at most 0.00002.
Values sent between devices are 32-bit elements; how exact they have to be, the bound alone decides.
No kernel may reach another device: no remote copies, remote signals or barrier semaphores. Data moves between devices by JAX's collectives and lax.ppermute only.
A program may use at most 64 MiB of HBM per device.

```python
import math
import jax
import jax.numpy as jnp

NZ = 128
STEPS = 5
NLAB = 8
NSRC = 64
NREC = 256
NX = 32
NY = 64


def smooth_modes(key, count, amp_lo, amp_hi, wave_lo, wave_hi):
    keys = jax.random.split(key, 4)
    lengths = jax.random.uniform(keys[0], (3, count, 3), jnp.float32, wave_lo, wave_hi)
    flips = jax.random.uniform(keys[1], (3, count, 3), jnp.float32)
    signs = jnp.where(flips < 0.5, -1.0, 1.0).astype(jnp.float32)
    waves = signs * (2.0 * math.pi) / lengths
    phases = jax.random.uniform(keys[2], (3, count), jnp.float32, 0.0, 2.0 * math.pi)
    amps = jax.random.uniform(keys[3], (3, count), jnp.float32, amp_lo, amp_hi)
    coord_x = jnp.arange(NX, dtype=jnp.float32)[:, None, None]
    coord_y = jnp.arange(NY, dtype=jnp.float32)[None, :, None]
    coord_z = jnp.arange(NZ, dtype=jnp.float32)[None, None, :]
    components = []
    for comp in range(3):
        total = jnp.zeros((NX, NY, NZ), jnp.float32)
        for mode in range(count):
            angle = waves[comp, mode, 0] * coord_x + waves[comp, mode, 1] * coord_y + waves[comp, mode, 2] * coord_z + phases[comp, mode]
            total = total + amps[comp, mode] * jnp.cos(angle)
        components.append(total)
    return jnp.stack(components)


def draw_wavefield(key, part):
    key_modes = jax.random.fold_in(key, 11)
    key_rough = jax.random.fold_in(key, 12)
    key_stress = jax.random.fold_in(key, 13)
    smooth = smooth_modes(key_modes, 4, 1.2, 1.8, 16.0, 48.0)
    rough = 0.2 * jnp.clip(jax.random.normal(key_rough, (3, NX, NY, NZ), jnp.float32), -6.0, 6.0)
    stress = 0.25 * jnp.clip(jax.random.normal(key_stress, (6, NX, NY, NZ), jnp.float32), -6.0, 6.0)
    return jnp.concatenate([smooth + rough, stress], axis=0).astype(jnp.float32)


def place_ends(array, rng, low, largest):
    shape = array.shape
    place = [jax.random.randint(jax.random.fold_in(rng, axis), (), 0, shape[axis]) for axis in range(len(shape))]
    array = array.at[tuple(place)].set(low)
    longest = shape.index(max(shape))
    place[longest] = (place[longest] + 1) % shape[longest]
    return array.at[tuple(place)].set(largest)


def normal_values(own_key, shape, spread, most, kind=jnp.bfloat16):
    return jnp.clip(spread * jax.random.normal(own_key, shape, jnp.float32), -most, most).astype(kind)


def setup_inputs(seed: int = 0, part: int = 0) -> dict:
    splits = jax.random.split(jax.random.key(seed), 9)
    part_splits = jax.random.split(jax.random.fold_in(splits[8], part), 9)
    return {
        "wavefield": draw_wavefield(jax.random.fold_in(jax.random.fold_in(splits[8], part), 71), part),
        "labels": place_ends(jax.random.randint(splits[1], (NX, NY, NZ), 0, NLAB), jax.random.fold_in(splits[1], 1), 0, NLAB - 1).astype(jnp.int32),
        "lame_table": jnp.clip(jnp.exp(jax.random.uniform(splits[2], (NLAB,), jnp.float32, math.log(0.5), math.log(2.0))), 0.5, 2.0),
        "shear_table": jnp.clip(jnp.exp(jax.random.uniform(splits[3], (NLAB,), jnp.float32, math.log(0.1), math.log(0.6))), 0.1, 0.6),
        "density_table": jnp.clip(jnp.exp(jax.random.uniform(splits[4], (NLAB,), jnp.float32, math.log(0.8), math.log(2.0))), 0.8, 2.0),
        "source_cells": place_ends(jax.random.randint(part_splits[5], (NSRC,), 0, NX * NY * NZ), jax.random.fold_in(part_splits[5], 1), 0, (NX * NY * NZ) - 1).astype(jnp.int32),
        "source_amps": normal_values(part_splits[6], (STEPS, NSRC), 1.0, 6.0, jnp.float32),
        "receiver_cells": place_ends(jax.random.randint(splits[7], (NREC,), 0, NX * NY * NZ), jax.random.fold_in(splits[7], 1), 0, (NX * NY * NZ) - 1).astype(jnp.int32),
    }


stencil_coeffs = (1225.0 / 1024.0, -245.0 / 3072.0, 49.0 / 5120.0, -5.0 / 7168.0)
time_step = 0.15
sponge_width = 16.0


def shifted(padded, offset, direction, layout):
    padding, margins, extent = layout
    pieces = []
    for dimension in range(3):
        start = padding[dimension] - margins[dimension] + (offset if dimension == direction else 0)
        pieces.append(slice(start, start + extent[dimension] + 2 * margins[dimension]))
    return padded[tuple(pieces)]


def derivative(padded, direction, forward, layout):
    result = None
    for number in range(1, 5):
        if forward:
            later, earlier = number, 1 - number
        else:
            later, earlier = number - 1, -number
        term = stencil_coeffs[number - 1] * (shifted(padded, later, direction, layout) - shifted(padded, earlier, direction, layout))
        result = term if result is None else result + term
    return result


def velocity_update(velocity, stress_padded, buoyancy, layout):
    normal_x, normal_y, normal_z = stress_padded[0], stress_padded[1], stress_padded[2]
    shear_xy, shear_xz, shear_yz = stress_padded[3], stress_padded[4], stress_padded[5]
    velocity_x = velocity[0] + time_step * buoyancy * (derivative(normal_x, 0, True, layout) + derivative(shear_xy, 1, False, layout) + derivative(shear_xz, 2, False, layout))
    velocity_y = velocity[1] + time_step * buoyancy * (derivative(shear_xy, 0, False, layout) + derivative(normal_y, 1, True, layout) + derivative(shear_yz, 2, False, layout))
    velocity_z = velocity[2] + time_step * buoyancy * (derivative(shear_xz, 0, False, layout) + derivative(shear_yz, 1, False, layout) + derivative(normal_z, 2, True, layout))
    return [velocity_x, velocity_y, velocity_z]


def stress_update(stress, velocity_padded, lame_first, shear, layout):
    velocity_x, velocity_y, velocity_z = velocity_padded[0], velocity_padded[1], velocity_padded[2]
    strain_x = derivative(velocity_x, 0, False, layout)
    strain_y = derivative(velocity_y, 1, False, layout)
    strain_z = derivative(velocity_z, 2, False, layout)
    volume = strain_x + strain_y + strain_z
    normal_x = stress[0] + time_step * (lame_first * volume + 2.0 * shear * strain_x)
    normal_y = stress[1] + time_step * (lame_first * volume + 2.0 * shear * strain_y)
    normal_z = stress[2] + time_step * (lame_first * volume + 2.0 * shear * strain_z)
    shear_xy = stress[3] + time_step * shear * (derivative(velocity_x, 1, True, layout) + derivative(velocity_y, 0, True, layout))
    shear_xz = stress[4] + time_step * shear * (derivative(velocity_x, 2, True, layout) + derivative(velocity_z, 0, True, layout))
    shear_yz = stress[5] + time_step * shear * (derivative(velocity_y, 2, True, layout) + derivative(velocity_z, 1, True, layout))
    return [normal_x, normal_y, normal_z, shear_xy, shear_xz, shear_yz]


def lookup(labels, table):
    result = jnp.zeros(labels.shape, jnp.float32)
    for label in range(table.shape[0]):
        result = result + jnp.where(labels == label, table[label], jnp.zeros((), table.dtype))
    return result


def profile(position, count):
    distance = jnp.minimum(position, count - 1 - position).astype(jnp.float32)
    depth = jnp.maximum(sponge_width - distance, 0.0) / sponge_width
    return jnp.exp(-(0.5 * depth) * (0.5 * depth))


def reference(wavefield, labels, lame_table, shear_table, density_table, source_cells, source_amps, receiver_cells):
    lame_first = lookup(labels, lame_table)
    shear = lookup(labels, shear_table)
    buoyancy = 1.0 / lookup(labels, density_table)
    damping = profile(jnp.arange(NX, dtype=jnp.int32), NX)[:, None, None] * profile(jnp.arange(NY, dtype=jnp.int32), NY)[None, :, None] * profile(jnp.arange(NZ, dtype=jnp.int32), NZ)[None, None, :]
    layout = ((4, 4, 4), (0, 0, 0), (NX, NY, NZ))
    source_x = source_cells // (NY * NZ)
    source_y = (source_cells // NZ) % NY
    source_z = source_cells % NZ
    probe_x = receiver_cells // (NY * NZ)
    probe_y = (receiver_cells // NZ) % NY
    probe_z = receiver_cells % NZ
    fields = [wavefield[number] for number in range(9)]
    rows = []
    for step in range(STEPS):
        padded_stress = [jnp.pad(field, 4) for field in fields[3:]]
        velocity = velocity_update(fields[:3], padded_stress, buoyancy, layout)
        padded_velocity = [jnp.pad(field, 4) for field in velocity]
        stress = stress_update(fields[3:], padded_velocity, lame_first, shear, layout)
        push = time_step * source_amps[step]
        for number in range(3):
            stress[number] = stress[number].at[source_x, source_y, source_z].add(push)
        fields = [field * damping for field in velocity + stress]
        pressure = -(fields[3][probe_x, probe_y, probe_z] + fields[4][probe_x, probe_y, probe_z] + fields[5][probe_x, probe_y, probe_z]) / 3.0
        rows.append(pressure)
    return jnp.stack(fields), jnp.stack(rows)
```

```python
import functools

import jax
import jax.numpy as jnp
from jax import lax
from jax.experimental import pallas as pl
from jax.experimental.pallas import tpu as pltpu
from jax.sharding import PartitionSpec as P

STEPS = 5
REACH = 4
PAD = 8

stencil_coeffs = (1225.0 / 1024.0, -245.0 / 3072.0, 49.0 / 5120.0, -5.0 / 7168.0)
time_step = 0.15
sponge_width = 16.0

VMEM = pl.BlockSpec(memory_space=pltpu.VMEM)
SMEM = pl.BlockSpec(memory_space=pltpu.SMEM)
ALONG_X = (3, 6, 7)
ALONG_Y = (4, 6, 8)


def combine(value, forward):
    result = None
    for number in range(1, 5):
        later, earlier = (number, 1 - number) if forward else (number - 1, -number)
        term = stencil_coeffs[number - 1] * (value(later) - value(earlier))
        result = term if result is None else result + term
    return result


def depth_derivative(plane, forward):
    depth = plane.shape[-1]
    lane = lax.broadcasted_iota(jnp.int32, plane.shape, len(plane.shape) - 1)

    def value(offset):
        if offset == 0:
            return plane
        turned = pltpu.roll(plane, (-offset) % depth, len(plane.shape) - 1)
        keep = lane < depth - offset if offset > 0 else lane >= -offset
        return jnp.where(keep, turned, 0.0)

    return combine(value, forward)


def put_slabs(sent, fields_x, fields_y):
    low_x, high_x, low_y, high_y = sent
    for number, (ref, index) in enumerate(fields_x):
        size_x = ref.shape[1]
        low_x[number] = ref[index, :REACH]
        high_x[number] = ref[index, size_x - REACH :]
    for number, (ref, index) in enumerate(fields_y):
        size_x, size_y = ref.shape[1:3]
        for x in range(size_x):
            rows = pl.ds((x % 2) * REACH, REACH)
            low_y[number, x // 2, rows, :] = ref[index, x, :REACH, :]
            high_y[number, x // 2, rows, :] = ref[index, x, size_y - REACH :, :]


def fill_padded(flags, got, wide_x, wide_y, cores_x, cores_y):
    from_low_x, from_high_x, from_low_y, from_high_y = got
    for number, (ref, index) in enumerate(cores_x):
        size_x = ref.shape[1]
        wide_x[number, :REACH] = jnp.where(flags[0] > 0, from_low_x[number], 0.0)
        wide_x[number, REACH + size_x :] = jnp.where(flags[1] > 0, from_high_x[number], 0.0)
        wide_x[number, REACH : REACH + size_x] = ref[index]
    for number, (ref, index) in enumerate(cores_y):
        size_x, size_y = ref.shape[1:3]
        wide_y[number, :, PAD : PAD + size_y, :] = ref[index]
        for x in range(size_x):
            rows = pl.ds((x % 2) * REACH, REACH)
            wide_y[number, x, PAD - REACH : PAD, :] = jnp.where(
                flags[2] > 0, from_low_y[number, x // 2, rows, :], 0.0
            )
            wide_y[number, x, PAD + size_y : PAD + size_y + REACH, :] = jnp.where(
                flags[3] > 0, from_high_y[number, x // 2, rows, :], 0.0
            )


def along_x(wide_x, number, x, forward):
    return combine(lambda offset: wide_x[number, REACH + x + offset], forward)


def along_y(wide_y, number, x, size_y, forward):
    return combine(
        lambda offset: wide_y[number, x, PAD + offset : PAD + offset + size_y, :], forward
    )


def slab_kernel(fields, *sent):
    put_slabs(
        sent, [(fields, index) for index in ALONG_X], [(fields, index) for index in ALONG_Y]
    )


def velocity_kernel(flags, fields, buoyancy, *rest):
    got, velocity, sent, (wide_x, wide_y) = rest[:4], rest[4], rest[5:9], rest[9:]
    size_x, size_y = fields.shape[1:3]
    fill_padded(
        flags,
        got,
        wide_x,
        wide_y,
        [(fields, index) for index in ALONG_X],
        [(fields, index) for index in ALONG_Y],
    )
    for x in range(size_x):
        factor = buoyancy[x]
        velocity[0, x] = fields[0, x] + factor * (
            along_x(wide_x, 0, x, True)
            + along_y(wide_y, 1, x, size_y, False)
            + depth_derivative(fields[7, x], False)
        )
        velocity[1, x] = fields[1, x] + factor * (
            along_x(wide_x, 1, x, False)
            + along_y(wide_y, 0, x, size_y, True)
            + depth_derivative(fields[8, x], False)
        )
        velocity[2, x] = fields[2, x] + factor * (
            along_x(wide_x, 2, x, False)
            + along_y(wide_y, 2, x, size_y, False)
            + depth_derivative(fields[5, x], True)
        )
    each = [(velocity, index) for index in range(3)]
    put_slabs(sent, each, each)


def stress_kernel(last, flags, fields, velocity, lame, shear, damping, source, lanes, rows, *rest):
    got, out, trace = rest[:4], rest[4], rest[5]
    sent = () if last else rest[6:10]
    wide_x, wide_y, pressure = rest[-3:]
    size_x, size_y, depth = fields.shape[1:]
    each = [(velocity, index) for index in range(3)]
    fill_padded(flags, got, wide_x, wide_y, each, each)
    for x in range(size_x):
        damp = damping[x]
        modulus = shear[x]
        strain_x = along_x(wide_x, 0, x, False)
        strain_y = along_y(wide_y, 1, x, size_y, False)
        strain_z = depth_derivative(velocity[2, x], False)
        common = lame[x] * (strain_x + strain_y + strain_z) + source[x]
        twice = 2.0 * modulus
        normal_x = (fields[3, x] + (common + twice * strain_x)) * damp
        normal_y = (fields[4, x] + (common + twice * strain_y)) * damp
        normal_z = (fields[5, x] + (common + twice * strain_z)) * damp
        out[3, x] = normal_x
        out[4, x] = normal_y
        out[5, x] = normal_z
        pressure[x] = normal_x + normal_y + normal_z
        out[6, x] = damp * (
            fields[6, x]
            + modulus * (along_y(wide_y, 0, x, size_y, True) + along_x(wide_x, 1, x, True))
        )
        out[7, x] = damp * (
            fields[7, x]
            + modulus * (depth_derivative(velocity[0, x], True) + along_x(wide_x, 2, x, True))
        )
        out[8, x] = damp * (
            fields[8, x]
            + modulus
            * (depth_derivative(velocity[1, x], True) + along_y(wide_y, 2, x, size_y, True))
        )
        for number in range(3):
            out[number, x] = velocity[number, x] * damp
    if not last:
        put_slabs(
            sent, [(out, index) for index in ALONG_X], [(out, index) for index in ALONG_Y]
        )
    picked = jnp.dot(
        pressure[...].reshape(size_x * size_y, depth),
        lanes[...],
        precision=lax.Precision.HIGHEST,
        preferred_element_type=jnp.float32,
    )
    trace[...] = jnp.sum(picked * rows[...], axis=0, keepdims=True) * (-1.0 / 3.0)


def ring(block, axis, step):
    count = lax.axis_size(axis)
    return lax.ppermute(block, axis, [(i, (i + step) % count) for i in range(count)])


def exchange(sent):
    low_x, high_x, low_y, high_y = sent
    return (
        ring(high_x, "gx", 1),
        ring(low_x, "gx", -1),
        ring(high_y, "gy", 1),
        ring(low_y, "gy", -1),
    )


def total_over(block, axis):
    count = lax.axis_size(axis)
    if count > 4:
        return lax.psum(block, axis)
    result = block
    for step in range(1, count):
        result = result + ring(block, axis, step)
    return result


def material_kernel(tables, labels, lame, shear, buoyancy):
    for x in range(labels.shape[0]):
        label = labels[x]
        values = [jnp.zeros(label.shape, jnp.float32)] * 3
        for entry in range(tables.shape[1]):
            here = label == entry
            values = [
                jnp.where(here, tables[row, entry], value) for row, value in enumerate(values)
            ]
        lame[x], shear[x], buoyancy[x] = values


def profile(position, count):
    distance = jnp.minimum(position, count - 1 - position).astype(jnp.float32)
    depth = jnp.maximum(sponge_width - distance, 0.0) / sponge_width
    return jnp.exp(-(0.5 * depth) * (0.5 * depth))


def body(
    wavefield,
    labels,
    lame_table,
    shear_table,
    density_table,
    source_cells,
    source_amps,
    receiver_cells,
):
    width_x, width_y, depth_z = labels.shape
    count_x, count_y = lax.axis_size("gx"), lax.axis_size("gy")
    total_x = width_x * count_x
    total_y = width_y * count_y
    place_x, place_y = lax.axis_index("gx"), lax.axis_index("gy")
    anchor_x = place_x * width_x
    anchor_y = place_y * width_y
    probes = receiver_cells.shape[0]

    f32 = lambda *shape: jax.ShapeDtypeStruct(shape, jnp.float32)
    slab_x = f32(3, REACH, width_y, depth_z)
    slab_y = f32(3, width_x // 2, 2 * REACH, depth_z)
    slabs = [slab_x, slab_x, slab_y, slab_y]
    wide = [
        pltpu.VMEM((3, width_x + 2 * REACH, width_y, depth_z), jnp.float32),
        pltpu.VMEM((3, width_x, width_y + 2 * PAD, depth_z), jnp.float32),
    ]

    sent = pl.pallas_call(
        slab_kernel, out_shape=slabs, in_specs=[VMEM], out_specs=[VMEM] * 4, name="slabs"
    )(wavefield)

    flags = jnp.stack(
        [place_x > 0, place_x < count_x - 1, place_y > 0, place_y < count_y - 1]
    ).astype(jnp.int32)
    tables = time_step * jnp.stack([lame_table, shear_table, 1.0 / density_table])
    lame, shear, buoyancy = pl.pallas_call(
        material_kernel,
        out_shape=[f32(*labels.shape)] * 3,
        in_specs=[SMEM, VMEM],
        out_specs=[VMEM] * 3,
        cost_estimate=pl.CostEstimate(
            flops=40 * labels.size, bytes_accessed=16 * labels.size, transcendentals=0
        ),
        name="materials",
    )(tables, labels)
    across_x = anchor_x + jnp.arange(width_x, dtype=jnp.int32)
    across_y = anchor_y + jnp.arange(width_y, dtype=jnp.int32)
    damping = (
        profile(across_x, total_x)[:, None, None]
        * profile(across_y, total_y)[None, :, None]
        * profile(jnp.arange(depth_z, dtype=jnp.int32), depth_z)[None, None, :]
    )

    def locate(cells):
        local_x = cells // (total_y * depth_z) - anchor_x
        local_y = cells // depth_z % total_y - anchor_y
        inside = (local_x >= 0) & (local_x < width_x) & (local_y >= 0) & (local_y < width_y)
        return jnp.where(inside, local_x * width_y + local_y, -1), cells % depth_z

    column = jnp.arange(width_x * width_y, dtype=jnp.int32)
    depths = jnp.arange(depth_z, dtype=jnp.int32)
    source_row, source_lane = locate(source_cells)
    pushes = jnp.where(
        source_row[None, None, :] == column[None, :, None],
        (time_step * source_amps)[:, None, :],
        0.0,
    ).reshape(STEPS * width_x * width_y, -1)
    sources = jnp.dot(
        pushes,
        (source_lane[:, None] == depths[None, :]).astype(jnp.float32),
        precision=lax.Precision.HIGHEST,
    ).reshape(STEPS, width_x, width_y, depth_z)
    probe_row, probe_lane = locate(receiver_cells)
    rows = (column[:, None] == probe_row[None, :]).astype(jnp.float32)
    lanes = (depths[:, None] == probe_lane[None, :]).astype(jnp.float32)

    block = (width_x, width_y, depth_z)
    cells = width_x * width_y * depth_z
    fields = wavefield
    traces = []
    for step in range(STEPS):
        last = step == STEPS - 1
        velocity, *sent = pl.pallas_call(
            velocity_kernel,
            out_shape=[f32(3, *block)] + slabs,
            in_specs=[SMEM] + [VMEM] * 6,
            out_specs=[VMEM] * 5,
            scratch_shapes=wide,
            cost_estimate=pl.CostEstimate(
                flops=120 * cells, bytes_accessed=64 * cells, transcendentals=0
            ),
            name="velocity",
        )(flags, fields, buoyancy, *exchange(sent))
        fields, trace, *sent = pl.pallas_call(
            functools.partial(stress_kernel, last),
            out_shape=[f32(9, *block), f32(1, probes)] + ([] if last else slabs),
            in_specs=[SMEM] + [VMEM] * 12,
            out_specs=[VMEM] * (2 if last else 6),
            scratch_shapes=wide + [pltpu.VMEM(block, jnp.float32)],
            cost_estimate=pl.CostEstimate(
                flops=150 * cells, bytes_accessed=64 * cells, transcendentals=0
            ),
            name="stress",
        )(
            flags,
            fields,
            velocity,
            lame,
            shear,
            damping,
            sources[step],
            lanes,
            rows,
            *exchange(sent),
        )
        traces.append(trace)
    parts = jnp.concatenate(traces, axis=0)
    return (fields, total_over(total_over(parts, "gy"), "gx"))


def solution(mesh):
    placed = (
        P(None, ("shot", "gx"), "gy", None),
        P("gx", "gy", None),
        P(),
        P(),
        P(),
        P("shot"),
        P(None, "shot"),
        P(),
    )
    return jax.shard_map(
        body,
        mesh=mesh,
        in_specs=placed,
        out_specs=(P(None, ("shot", "gx"), "gy", None), P(None, "shot")),
        check_vma=False,
    )
```

```python
import functools

import jax
import jax.numpy as jnp
from jax import lax
from jax.experimental import pallas as pl
from jax.experimental.pallas import tpu as pltpu
from jax.sharding import PartitionSpec as P

STEPS = 5
REACH = 4
PAD = 8

stencil_coeffs = (1225.0 / 1024.0, -245.0 / 3072.0, 49.0 / 5120.0, -5.0 / 7168.0)
time_step = 0.15
sponge_width = 16.0

PARAMS = pltpu.CompilerParams(vmem_limit_bytes=12 * 1024 * 1024)
VMEM = pl.BlockSpec(memory_space=pltpu.VMEM)
SMEM = pl.BlockSpec(memory_space=pltpu.SMEM)
ALONG_X = (3, 6, 7)
ALONG_Y = (4, 6, 8)


def combine(value, forward):
    result = None
    for number in range(1, 5):
        later, earlier = (number, 1 - number) if forward else (number - 1, -number)
        term = stencil_coeffs[number - 1] * (value(later) - value(earlier))
        result = term if result is None else result + term
    return result


def depth_derivative(plane, forward):
    depth = plane.shape[-1]
    lane = lax.broadcasted_iota(jnp.int32, plane.shape, len(plane.shape) - 1)

    def value(offset):
        if offset == 0:
            return plane
        turned = pltpu.roll(plane, (-offset) % depth, len(plane.shape) - 1)
        keep = lane < depth - offset if offset > 0 else lane >= -offset
        return jnp.where(keep, turned, 0.0)

    return combine(value, forward)


def put_slabs(sent, fields_x, fields_y):
    low_x, high_x, low_y, high_y = sent
    for number, (ref, index) in enumerate(fields_x):
        size_x = ref.shape[1]
        low_x[number] = ref[index, :REACH]
        high_x[number] = ref[index, size_x - REACH :]
    for number, (ref, index) in enumerate(fields_y):
        size_x, size_y = ref.shape[1:3]
        for x in range(size_x):
            rows = pl.ds((x % 2) * REACH, REACH)
            low_y[number, x // 2, rows, :] = ref[index, x, :REACH, :]
            high_y[number, x // 2, rows, :] = ref[index, x, size_y - REACH :, :]


def own_x(ref, index, x, forward):
    size_x = ref.shape[1]
    result = None
    for offset, factor in taps(forward):
        if 0 <= x + offset < size_x:
            term = factor * ref[index, x + offset]
            result = term if result is None else result + term
    return result


def fill_wide(wide, cores):
    for number, (ref, index) in enumerate(cores):
        size_x, size_y, depth = ref.shape[1:]
        margin = jnp.zeros((size_x, PAD, depth), jnp.float32)
        wide[number, :, :PAD, :] = margin
        wide[number, :, PAD + size_y :, :] = margin
        wide[number, :, PAD : PAD + size_y, :] = ref[index]


def own_y(wide, number, x, size_y, forward):
    return combine(
        lambda offset: wide[number, x, PAD + offset : PAD + offset + size_y, :], forward
    )


def taps(forward):
    result = []
    for number in range(1, 5):
        later, earlier = (number, 1 - number) if forward else (number - 1, -number)
        result += [(later, stencil_coeffs[number - 1]), (earlier, -stencil_coeffs[number - 1])]
    return result


def fill_edges(flags, from_low_y, from_high_y, below, above):
    below[...] = jnp.zeros(below.shape, jnp.float32)
    above[...] = jnp.zeros(above.shape, jnp.float32)
    for number in range(below.shape[0]):
        for x in range(below.shape[1]):
            rows = pl.ds((x % 2) * REACH, REACH)
            below[number, x, PAD - REACH : PAD, :] = jnp.where(
                flags[2, :REACH] > 0, from_low_y[number, x // 2, rows, :], 0.0
            )
            above[number, x, PAD : PAD + REACH, :] = jnp.where(
                flags[3, :REACH] > 0, from_high_y[number, x // 2, rows, :], 0.0
            )


def halo_x(flags, from_low_x, from_high_x, number, row, size_x):
    rows = slice(row, row + PAD)
    low = [jnp.where(flags[0] > 0, from_low_x[number, i, rows, :], 0.0) for i in range(REACH)]
    high = [jnp.where(flags[1] > 0, from_high_x[number, i, rows, :], 0.0) for i in range(REACH)]

    def part(x, forward):
        result = jnp.zeros_like(low[0])
        for offset, factor in taps(forward):
            if x + offset < 0:
                result = result + factor * low[x + offset + REACH]
            elif x + offset >= size_x:
                result = result + factor * high[x + offset - size_x]
        return result

    return part


def halo_y(below, above, number, row, size_y):
    def part(x, forward):
        result = jnp.zeros((PAD, below.shape[-1]), jnp.float32)
        for offset, factor in taps(forward):
            if row == 0 and offset < 0:
                result = result + factor * below[number, x, PAD + offset : 2 * PAD + offset, :]
            if row == size_y - PAD and offset > 0:
                result = result + factor * above[number, x, offset : PAD + offset, :]
        return result

    return part


def pick(pressure, lanes, rows):
    size_x, size_y, depth = pressure.shape
    picked = jnp.dot(
        pressure.reshape(size_x * size_y, depth),
        lanes,
        precision=lax.Precision.HIGHEST,
        preferred_element_type=jnp.float32,
    )
    return jnp.sum(picked * rows, axis=0, keepdims=True) * (-1.0 / 3.0)


def slab_kernel(fields, *sent):
    put_slabs(
        sent, [(fields, index) for index in ALONG_X], [(fields, index) for index in ALONG_Y]
    )


def velocity_own_kernel(base, old, stress, buoyancy, *rest):
    size_x, size_y = stress.shape[1:3]
    xx, yy, zz, xy, xz, yz = range(base, base + 6)
    if base == 0:
        lanes, rows, velocity, trace, wide = rest
    else:
        velocity, wide = rest
    fill_wide(wide, [(stress, yy), (stress, xy), (stress, yz)])
    for x in range(size_x):
        factor = buoyancy[x]
        velocity[0, x] = old[0, x] + factor * (
            own_x(stress, xx, x, True)
            + own_y(wide, 1, x, size_y, False)
            + depth_derivative(stress[xz, x], False)
        )
        velocity[1, x] = old[1, x] + factor * (
            own_x(stress, xy, x, False)
            + own_y(wide, 0, x, size_y, True)
            + depth_derivative(stress[yz, x], False)
        )
        velocity[2, x] = old[2, x] + factor * (
            own_x(stress, xz, x, False)
            + own_y(wide, 2, x, size_y, False)
            + depth_derivative(stress[zz, x], True)
        )
    if base == 0:
        trace[...] = pick(stress[0] + stress[1] + stress[2], lanes[...], rows[...])


def velocity_halo_kernel(flags, partial, buoyancy, low_x, high_x, low_y, high_y, *rest):
    velocity, sent, (below, above) = rest[0], rest[1:5], rest[5:]
    size_x, size_y = partial.shape[1:3]
    fill_edges(flags, low_y, high_y, below, above)
    for row in range(0, size_y, PAD):
        rows = slice(row, row + PAD)
        for number, number_y, forward_x, forward_y in (
            (0, 1, True, False),
            (1, 0, False, True),
            (2, 2, False, False),
        ):
            part_x = halo_x(flags, low_x, high_x, number, row, size_x)
            part_y = halo_y(below, above, number_y, row, size_y)
            for x in range(size_x):
                velocity[number, x, rows, :] = partial[number, x, rows, :] + buoyancy[
                    x, rows, :
                ] * (part_x(x, forward_x) + part_y(x, forward_y))
    each = [(velocity, index) for index in range(3)]
    put_slabs(sent, each, each)


def stress_own_kernel(base, old, velocity, lame, shear, damping, source, out, damped, wide):
    size_x, size_y = velocity.shape[1:3]
    fill_wide(wide, [(velocity, index) for index in range(3)])
    for x in range(size_x):
        damp = damping[x]
        lame_here = lame[x]
        modulus = shear[x]
        strain_x = own_x(velocity, 0, x, False)
        strain_y = own_y(wide, 1, x, size_y, False)
        strain_z = depth_derivative(velocity[2, x], False)
        common = lame_here * (strain_x + strain_y + strain_z) + damp * source[x]
        twice = 2.0 * modulus
        out[0, x] = damp * old[base, x] + (common + twice * strain_x)
        out[1, x] = damp * old[base + 1, x] + (common + twice * strain_y)
        out[2, x] = damp * old[base + 2, x] + (common + twice * strain_z)
        out[3, x] = damp * old[base + 3, x] + modulus * (
            own_y(wide, 0, x, size_y, True) + own_x(velocity, 1, x, True)
        )
        out[4, x] = damp * old[base + 4, x] + modulus * (
            depth_derivative(velocity[0, x], True) + own_x(velocity, 2, x, True)
        )
        out[5, x] = damp * old[base + 5, x] + modulus * (
            depth_derivative(velocity[1, x], True) + own_y(wide, 2, x, size_y, True)
        )
        for number in range(3):
            damped[number, x] = velocity[number, x] * damp


def stress_halo_kernel(last, flags, partial, lame, shear, low_x, high_x, low_y, high_y, *rest):
    if last:
        damped, lanes, mask, out, trace, below, above = rest
        base = 3
        for number in range(3):
            out[number] = damped[number]
    else:
        out, sent, (below, above) = rest[0], rest[1:5], rest[5:]
        base = 0
    size_x, size_y = partial.shape[1:3]
    fill_edges(flags, low_y, high_y, below, above)
    for row in range(0, size_y, PAD):
        rows = slice(row, row + PAD)
        along_x = [halo_x(flags, low_x, high_x, n, row, size_x) for n in range(3)]
        along_y = [halo_y(below, above, n, row, size_y) for n in range(3)]
        for x in range(size_x):
            modulus = shear[x, rows, :]
            strain_x, strain_y = along_x[0](x, False), along_y[1](x, False)
            common = lame[x, rows, :] * (strain_x + strain_y)
            twice = 2.0 * modulus
            changes = (
                common + twice * strain_x,
                common + twice * strain_y,
                common,
                modulus * (along_y[0](x, True) + along_x[1](x, True)),
                modulus * along_x[2](x, True),
                modulus * along_y[2](x, True),
            )
            for number, change in enumerate(changes):
                out[base + number, x, rows, :] = partial[number, x, rows, :] + change
    if last:
        trace[...] = pick(out[3] + out[4] + out[5], lanes[...], mask[...])
    else:
        put_slabs(
            sent, [(out, index - 3) for index in ALONG_X], [(out, index - 3) for index in ALONG_Y]
        )


def ring(block, axis, step):
    count = lax.axis_size(axis)
    return lax.ppermute(block, axis, [(i, (i + step) % count) for i in range(count)])


def exchange(sent):
    low_x, high_x, low_y, high_y = sent
    return (
        ring(high_x, "gx", 1),
        ring(low_x, "gx", -1),
        ring(high_y, "gy", 1),
        ring(low_y, "gy", -1),
    )


def total_over(block, axis):
    count = lax.axis_size(axis)
    if count > 4:
        return lax.psum(block, axis)
    result = block
    for step in range(1, count):
        result = result + ring(block, axis, step)
    return result


def material_kernel(tables, labels, damping, lame, shear, buoyancy):
    for x in range(labels.shape[0]):
        label = labels[x]
        values = [jnp.zeros(label.shape, jnp.float32)] * 3
        for entry in range(tables.shape[1]):
            here = label == entry
            values = [
                jnp.where(here, tables[row, entry], value) for row, value in enumerate(values)
            ]
        lame[x] = values[0] * damping[x]
        shear[x] = values[1] * damping[x]
        buoyancy[x] = values[2]


def profile(position, count):
    distance = jnp.minimum(position, count - 1 - position).astype(jnp.float32)
    depth = jnp.maximum(sponge_width - distance, 0.0) / sponge_width
    return jnp.exp(-(0.5 * depth) * (0.5 * depth))


def body(
    wavefield,
    labels,
    lame_table,
    shear_table,
    density_table,
    source_cells,
    source_amps,
    receiver_cells,
):
    width_x, width_y, depth_z = labels.shape
    count_x, count_y = lax.axis_size("gx"), lax.axis_size("gy")
    total_x = width_x * count_x
    total_y = width_y * count_y
    place_x, place_y = lax.axis_index("gx"), lax.axis_index("gy")
    anchor_x = place_x * width_x
    anchor_y = place_y * width_y
    probes = receiver_cells.shape[0]

    f32 = lambda *shape: jax.ShapeDtypeStruct(shape, jnp.float32)
    slab_x = f32(3, REACH, width_y, depth_z)
    slab_y = f32(3, width_x // 2, 2 * REACH, depth_z)
    slabs = [slab_x, slab_x, slab_y, slab_y]
    wide = [pltpu.VMEM((3, width_x, width_y + 2 * PAD, depth_z), jnp.float32)]
    edges = [pltpu.VMEM((3, width_x, 2 * PAD, depth_z), jnp.float32)] * 2

    sent = pl.pallas_call(
        slab_kernel, out_shape=slabs, in_specs=[VMEM], out_specs=[VMEM] * 4, name="slabs", compiler_params=PARAMS
    )(wavefield)

    inner = [place_x > 0, place_x < count_x - 1, place_y > 0, place_y < count_y - 1]
    flags = jnp.broadcast_to(
        jnp.stack(inner).astype(jnp.float32)[:, None, None], (4, PAD, depth_z)
    )
    across_x = anchor_x + jnp.arange(width_x, dtype=jnp.int32)
    across_y = anchor_y + jnp.arange(width_y, dtype=jnp.int32)
    damping = (
        profile(across_x, total_x)[:, None, None]
        * profile(across_y, total_y)[None, :, None]
        * profile(jnp.arange(depth_z, dtype=jnp.int32), depth_z)[None, None, :]
    )
    tables = time_step * jnp.stack([lame_table, shear_table, 1.0 / density_table])
    lame, shear, buoyancy = pl.pallas_call(
        material_kernel,
        out_shape=[f32(*labels.shape)] * 3,
        in_specs=[SMEM, VMEM, VMEM],
        out_specs=[VMEM] * 3,
        cost_estimate=pl.CostEstimate(
            flops=40 * labels.size, bytes_accessed=16 * labels.size, transcendentals=0
        ),
        name="materials", compiler_params=PARAMS,
    )(tables, labels, damping)
    def locate(cells):
        local_x = cells // (total_y * depth_z) - anchor_x
        local_y = cells // depth_z % total_y - anchor_y
        inside = (local_x >= 0) & (local_x < width_x) & (local_y >= 0) & (local_y < width_y)
        return jnp.where(inside, local_x * width_y + local_y, -1), cells % depth_z

    column = jnp.arange(width_x * width_y, dtype=jnp.int32)
    depths = jnp.arange(depth_z, dtype=jnp.int32)
    source_row, source_lane = locate(source_cells)
    pushes = jnp.where(
        source_row[None, None, :] == column[None, :, None],
        (time_step * source_amps)[:, None, :],
        0.0,
    ).reshape(STEPS * width_x * width_y, -1)
    sources = jnp.dot(
        pushes,
        (source_lane[:, None] == depths[None, :]).astype(jnp.float32),
        precision=lax.Precision.HIGHEST,
    ).reshape(STEPS, width_x, width_y, depth_z)
    probe_row, probe_lane = locate(receiver_cells)
    rows = (column[:, None] == probe_row[None, :]).astype(jnp.float32)
    lanes = (depths[:, None] == probe_lane[None, :]).astype(jnp.float32)

    block = (width_x, width_y, depth_z)
    cells = width_x * width_y * depth_z
    cost = lambda work: pl.CostEstimate(
        flops=work * cells, bytes_accessed=work * cells // 2, transcendentals=0
    )
    old, stress, base = wavefield, wavefield, 3
    traces = []
    for step in range(STEPS):
        last = step == STEPS - 1
        got = exchange(sent)
        partial, *trace = pl.pallas_call(
            functools.partial(velocity_own_kernel, base),
            out_shape=[f32(3, *block)] + ([] if base else [f32(1, probes)]),
            in_specs=[VMEM] * (3 if base else 5),
            out_specs=[VMEM] * (1 if base else 2),
            scratch_shapes=wide,
            cost_estimate=cost(120),
            name="velocity_own", compiler_params=PARAMS,
        )(old, stress, buoyancy, *(() if base else (lanes, rows)))
        traces += trace
        velocity, *sent = pl.pallas_call(
            velocity_halo_kernel,
            out_shape=[f32(3, *block)] + slabs,
            in_specs=[VMEM] * 7,
            out_specs=[VMEM] * 5,
            scratch_shapes=edges,
            cost_estimate=cost(40),
            name="velocity_halo", compiler_params=PARAMS,
        )(flags, partial, buoyancy, *got)
        got = exchange(sent)
        partial, old = pl.pallas_call(
            functools.partial(stress_own_kernel, base),
            out_shape=[f32(6, *block), f32(3, *block)],
            in_specs=[VMEM] * 6,
            out_specs=[VMEM] * 2,
            scratch_shapes=wide,
            cost_estimate=cost(150),
            name="stress_own", compiler_params=PARAMS,
        )(stress, velocity, lame, shear, damping, sources[step])
        stress, *sent = pl.pallas_call(
            functools.partial(stress_halo_kernel, last),
            out_shape=[f32(9, *block), f32(1, probes)] if last else [f32(6, *block)] + slabs,
            in_specs=[VMEM] * (11 if last else 8),
            out_specs=[VMEM] * (2 if last else 5),
            scratch_shapes=edges,
            cost_estimate=cost(50),
            name="stress_halo", compiler_params=PARAMS,
        )(flags, partial, lame, shear, *got, *((old, lanes, rows) if last else ()))
        base = 0
    fields = stress
    traces += sent
    parts = jnp.concatenate(traces, axis=0)
    return (fields, total_over(total_over(parts, "gy"), "gx"))


def solution(mesh):
    placed = (
        P(None, ("shot", "gx"), "gy", None),
        P("gx", "gy", None),
        P(),
        P(),
        P(),
        P("shot"),
        P(None, "shot"),
        P(),
    )
    return jax.shard_map(
        body,
        mesh=mesh,
        in_specs=placed,
        out_specs=(P(None, ("shot", "gx"), "gy", None), P(None, "shot")),
        check_vma=False,
    )
```
